32 devices in a mesh: gx: 4 (over y, x), gy: 4 (over z), gz: 2 (over core).
Axes of the slice: x: 2, y: 2, z: 4, core: 2. Of those that a mesh axis runs over, the one named last changes fastest.
Arguments:
- charges: float32 [128, 256, 256], P('gx', 'gy', 'gz'), may hold values from -8 to 8
- kernel_taps: float32 [5, 3, 17], replicated, may hold values from 0.08 to 0.4
Outputs:
- potential: float32 [128, 256, 256], P('gx', 'gy', 'gz')
The draws below stay inside these ranges and needn't reach their ends.
All inputs are finite; a program needn't handle non-finite values.
Results may differ from the reference program's by a relative error of at most 0.00029.
Values sent between devices are 32-bit elements; how exact they have to be, the bound alone decides.
A program may use at most 128 MiB of HBM per device.

```python
import math
import jax
import jax.numpy as jnp
from jax import lax

LEVELS = 5
TAPS = 17
NX = 128
NY = 256
NZ = 256


def block_levels(stream_key, shape, cuts, smallest, top_value):
    def one(dim, blocks):
        steps = jax.random.uniform(jax.random.fold_in(jax.random.fold_in(stream_key, 6), dim), (blocks,), jnp.float32, smallest / len(cuts), top_value / len(cuts))
        return jnp.repeat(jnp.exp(steps), shape[dim] // blocks).reshape((-1,) + (1,) * (len(shape) - dim - 1))

    loudness = one(*cuts[0])
    for cut in cuts[1:]:
        loudness = loudness * one(*cut)
    return loudness


def normal_values(stream_key, shape, width, most, shards=(), kind=jnp.bfloat16):
    factor_of = block_levels(stream_key, shape, shards, -0.22, 0.18) if shards else 1.0
    values = jax.random.normal(stream_key, shape, jnp.float32) * width * factor_of
    return jnp.minimum(jnp.maximum(values, -most), most).astype(kind)


def setup_inputs(seed: int = 0) -> dict:
    arg_keys = jax.random.split(jax.random.key(seed), 3)
    charges = normal_values(arg_keys[0], (NX, NY, NZ), 1.0, 8.0, ((0, 4), (1, 4), (2, 2)), jnp.float32)
    kernel_taps = jnp.clip(jnp.exp(jax.random.uniform(arg_keys[1], (LEVELS, 3, TAPS), jnp.float32, math.log(0.08), math.log(0.4))), 0.08, 0.4)
    return dict(charges=charges, kernel_taps=kernel_taps)


CUBIC = (-0.0625, 0.0, 0.5625, 1.0, 0.5625, 0.0, -0.0625)
PATTERNS = ("ij,jbc->ibc", "ij,ajc->aic", "ij,abj->abi")


def picks_matrix(weights, offsets):
    count = weights.shape[0]
    picks = (offsets[None, :, :] == jnp.arange(count, dtype=jnp.int32)[:, None, None]).astype(jnp.float32)
    return jnp.sum(weights.astype(jnp.float32)[:, None, None] * picks, axis=0)


def apply_axis(matrix, values, axis):
    return jnp.einsum(PATTERNS[axis], matrix, values, precision=lax.Precision.HIGHEST)


def stencil_padded(padded, taps_level):
    for axis in range(3):
        length = padded.shape[axis] - 16
        total = jnp.zeros(padded.shape[:axis] + (length,) + padded.shape[axis + 1:], jnp.float32)
        for offset in range(17):
            total = total + taps_level[axis, offset] * lax.slice_in_dim(padded, offset, offset + length, 1, axis)
        padded = total
    return padded


def restrict_padded(padded):
    cubic = jnp.array(CUBIC, jnp.float32)
    for axis in range(3):
        length = padded.shape[axis] - 6
        offsets = jnp.arange(length + 6, dtype=jnp.int32)[None, :] - 2 * jnp.arange(length // 2, dtype=jnp.int32)[:, None]
        padded = apply_axis(picks_matrix(cubic, offsets), padded, axis)
    return padded


def prolong_padded(padded):
    cubic = jnp.array(CUBIC, jnp.float32)
    for axis in range(3):
        length = padded.shape[axis] - 4
        offsets = 7 + jnp.arange(2 * length, dtype=jnp.int32)[:, None] - 2 * jnp.arange(length + 4, dtype=jnp.int32)[None, :]
        padded = apply_axis(picks_matrix(cubic, offsets), padded, axis)
    return padded


def reference(charges, kernel_taps):
    levels_charge = [charges]
    for level in range(1, LEVELS):
        levels_charge.append(restrict_padded(jnp.pad(levels_charge[-1], 3)))
    result = stencil_padded(jnp.pad(levels_charge[LEVELS - 1], 8), kernel_taps[LEVELS - 1])
    for level in range(LEVELS - 2, -1, -1):
        result = stencil_padded(jnp.pad(levels_charge[level], 8), kernel_taps[level]) + prolong_padded(jnp.pad(result, 2))
    return result
```

```python
import functools

import jax
import jax.numpy as jnp
from jax import lax
from jax.experimental import pallas as pl
from jax.experimental.pallas import tpu as pltpu
from jax.sharding import PartitionSpec as P

F32, BF16 = jnp.float32, jnp.bfloat16
LANES = 128
AXES = ("gx", "gy", "gz")
ODD = (-0.0625, 0.5625, 0.5625, -0.0625)
SIDES = tuple((a, b) for a in (-1, 0, 1) for b in (-1, 0, 1) if (a, b) != (0, 0))


def split(v):
    hi = v.astype(BF16)
    return hi, (v - hi.astype(F32)).astype(BF16)


def mm(a, b):
    return jnp.dot(a, b, preferred_element_type=F32)


def exact(a, b):
    return jnp.dot(a, b, preferred_element_type=F32, precision=lax.Precision.HIGHEST)


def dot_right(v, w):
    hi, lo = split(v)
    out = mm(hi, w[0][...]) + mm(lo, w[0][...])
    return out if w[1] is None else out + mm(hi, w[1][...])


def dot_left(w_ref, v, terms):
    hi, lo = split(v)
    return mm(w_ref[...], jnp.concatenate([hi, lo, hi][:terms], axis=0))


def grids(rows, cols):
    return (
        lax.broadcasted_iota(jnp.int32, (rows, cols), 0),
        lax.broadcasted_iota(jnp.int32, (rows, cols), 1),
    )


def pick(taps, level, axis, diff, ok):
    out = jnp.zeros(diff.shape, F32)
    for t in range(17):
        out = jnp.where(diff == t, taps[level, axis, t], out)
    return jnp.where(ok, out, 0.0)


def cubic(diff, ok):
    d = jnp.abs(diff)
    out = jnp.where(d == 0, 1.0, jnp.where(d == 1, 0.5625, jnp.where(d == 3, -0.0625, 0.0)))
    return jnp.where(ok, out, 0.0).astype(F32)


def up(n, m):
    return -(-n // m) * m


def inside(v, n):
    return (v >= 0) & (v < n)


def kernel(counts, dims, taps, x_ref, out_ref, e0, l0, r0, y0, y1, e1, l1, r1, t1, s1, g2, u2, y2, p2, d1,
           w0h, w0l, m0, w1h, w1l, m1, w2h, w2l, m2, c2, pz2, py2, pz1, py1,
           sa, ra, sza, rza, sb, rb, szb, rzb, sg, rg):
    nx, ny, nz = counts
    bx, by, bz = dims
    here = tuple(lax.axis_index(a) for a in AXES)
    gx, gy, gz = here
    cx, cy, cz = bx // 2, by // 2, bz // 2
    fx, fy, fz = bx // 4, by // 4, bz // 4

    def there(dx, dy, dz):
        return inside(gx + dx, nx) & inside(gy + dy, ny) & inside(gz + dz, nz)

    partners = [(a, b, 0) for a, b in SIDES] + [(0, 0, -1), (0, 0, 1)]
    for dim, n in enumerate(counts):
        for d in range(2, n):
            for sgn in (-d, d):
                partners.append(tuple(sgn if k == dim else 0 for k in range(3)))
    barrier = pltpu.get_barrier_semaphore()
    total = jnp.int32(0)
    for p in partners:
        ok = there(*p)
        total = total + ok.astype(jnp.int32)

        @pl.when(ok)
        def _(p=p):
            pl.semaphore_signal(
                barrier, inc=1, device_id=(gx + p[0], gy + p[1], gz + p[2]),
                device_id_type=pl.DeviceIdType.MESH,
            )

    def zero_halo(ref, wx, wy, mx, my):
        for a, b in SIDES:
            @pl.when(jnp.logical_not(there(a, b, 0)))
            def _(a=a, b=b):
                xs = {-1: (0, wx), 0: (wx, mx), 1: (wx + mx, wx)}[a]
                ys = {-1: (0, wy), 0: (wy, my), 1: (wy + my, wy)}[b]
                ref[pl.ds(*xs), pl.ds(*ys), :] = jnp.zeros((xs[1], ys[1], LANES), F32)

    zero_halo(e0, 8, 8, bx, by)
    zero_halo(e1, 5, 16, cx // 2, cy)
    pl.semaphore_wait(barrier, total)

    def exchange(src, base, ref, wx, wy, mx, my, send, recv):
        out = []
        for k, (a, b) in enumerate(SIDES):
            sx = {-1: (0, wx), 0: (0, mx), 1: (mx - wx, wx)}[a]
            sy = {-1: (0, wy), 0: (0, my), 1: (my - wy, wy)}[b]
            tx = {-1: (wx + mx, wx), 0: (wx, mx), 1: (0, wx)}[a]
            ty = {-1: (wy + my, wy), 0: (wy, my), 1: (0, wy)}[b]
            copy = pltpu.make_async_remote_copy(
                src_ref=src.at[pl.ds(base[0] + sx[0], sx[1]), pl.ds(base[1] + sy[0], sy[1]), :],
                dst_ref=ref.at[pl.ds(*tx), pl.ds(*ty), :],
                send_sem=send.at[k], recv_sem=recv.at[k],
                device_id=(gx + a, gy + b, gz), device_id_type=pl.DeviceIdType.MESH,
            )
            out.append((there(a, b, 0), there(-a, -b, 0), copy))
        return out

    def across(src, base, left, right, ranges, send, recv):
        out = []
        for k, (ofs, xs, ys) in enumerate(ranges):
            for h, (dz, dst) in enumerate(((1, left), (-1, right))):
                source = (src if k == 0 else base)
                copy = pltpu.make_async_remote_copy(
                    src_ref=source.at[pl.ds(xs[0] - ofs[0], xs[1]), pl.ds(ys[0] - ofs[1], ys[1]), :],
                    dst_ref=dst.at[pl.ds(*xs), pl.ds(*ys), :],
                    send_sem=send.at[k, h], recv_sem=recv.at[k, h],
                    device_id=(gx, gy, gz + dz), device_id_type=pl.DeviceIdType.MESH,
                )
                out.append((there(0, 0, dz), there(0, 0, -dz), copy))
        return out

    def start(copies):
        for to, _, copy in copies:
            pl.when(to)(copy.start)

    def arrive(copies):
        for _, fro, copy in copies:
            pl.when(fro)(copy.wait_recv)

    def left_over(copies):
        for to, _, copy in copies:
            pl.when(to)(copy.wait_send)

    def pieces(wx, wy, mx, my, direct):
        o = (wx, wy) if direct else (0, 0)
        n = (0, 0)
        return [
            (o, (wx, mx), (wy, my)),
            (n, (0, wx), (0, my + 2 * wy)),
            (n, (wx + mx, wx), (0, my + 2 * wy)),
            (n, (wx, mx), (0, wy)),
            (n, (wx, mx), (wy + my, wy)),
        ]

    xa = exchange(x_ref, (0, 0), e0, 8, 8, bx, by, sa, ra)
    za = across(x_ref, e0, l0, r0, pieces(8, 8, bx, by, True), sza, rza)
    start(xa)
    start(za[:2])
    e0[pl.ds(8, bx), pl.ds(8, by), :] = x_ref[...]

    def put(h, l, v):
        hi, lo = split(v)
        h[...] = hi
        if l is not None:
            l[...] = lo

    def stack(ref, v, terms):
        hi, lo = split(v)
        ref[...] = jnp.concatenate([hi, hi, lo][:terms], axis=1)

    i, j = grids(2 * bz, bz)
    pos = jnp.where(i < bz + bz // 2, i, i - 2 * bz)
    k0 = pick(taps, 0, 2, pos - j + 8, inside(pos, bz + 8) | inside(pos + 8, 8))
    rz = cubic(pos - 2 * j, j < cz)
    put(w0h, w0l, jnp.concatenate([k0, rz], axis=1))
    i, j = grids(by + cy, by + 16)
    stack(m0, jnp.where(i < by, pick(taps, 0, 1, j - i, i < by), cubic(j - 8 - 2 * (i - by), i >= by)), 3)
    i, j = grids(2 * cz, LANES)
    pos = jnp.where(i < cz + cz // 2, i, i - 2 * cz)
    kk = j - 2
    top = cz + 4
    ok = (j < top) & inside(gz * cz + kk, nz * cz)
    rlane = LANES - fz
    put(w1h, w1l, pick(taps, 1, 2, pos - kk + 8, ok) + cubic(pos - 2 * (j - rlane), j >= rlane))
    ry1 = up(cy + 4, 8)
    i, j = grids(ry1 + fy, cy + 32)
    ok = (i < cy + 4) & inside(gy * cy + i - 2, ny * cy)
    stack(m1, pick(taps, 1, 1, j - 16 - (i - 2) + 8, ok) + cubic(j - 16 - 2 * (i - ry1), i >= ry1), 3)
    def plain(axis, level, n, pad, turned):
        i, j = grids(pad, pad)
        d = (i - j if turned else j - i) + 8
        return pick(taps, level, axis, d, (i < n) & (j < n))

    def rest(n, pad, big, turned_r):
        i, j = grids(*((big, pad) if turned_r else (pad, big)))
        c, f = (j, i) if turned_r else (i, j)
        return cubic(f - 2 * c, (c < n) & (f < 2 * n))

    def operators(axis, n2, first, rows, count):
        n3, n4 = n2 // 2, n2 // 4
        q = up(n2, LANES)
        i, j = grids(rows, q)
        g = first + i
        ok = (i < count) & inside(g, n2)
        one = pick(taps, 2, axis, j - g + 8, ok & (j < n2))
        pr = cubic(g - 2 * j, ok & (j < n3))
        r23, r34 = rest(n3, q, q, False), rest(n4, q, q, False)
        p34 = rest(n4, q, q, True)
        two = exact(exact(pr, plain(axis, 3, n3, q, False)), r23)
        three = exact(exact(exact(exact(pr, p34), plain(axis, 4, n4, q, False)), r34), r23)
        return one, two, three

    n2x, n2y, n2z = nx * fx, ny * fy, nz * fz
    ez, ey, ex = fz + 5, fy + 5, fx + 5
    tz = 40
    row = lax.broadcasted_iota(jnp.int32, (LANES, 1), 0)
    ops = operators(2, n2z, gz * fz - 2, tz, ez)
    cols = jnp.concatenate(list(ops) + [jnp.zeros((LANES - 3 * tz, ops[0].shape[1]), F32)], axis=0)
    put(w2h, w2l, cols.T)
    ty = up(ey, 8)
    ops = operators(1, n2y, gy * fy - 2, ty, ey)
    stack(m2, jnp.concatenate(list(ops), axis=0)[:, :n2y], 3)
    tx = up(ex, 8)
    ops = operators(0, n2x, gx * fx - 2, tx, ex)
    lane = lax.broadcasted_iota(jnp.int32, (1, LANES), 1)
    tall = [o.T for o in ops]
    for r in range(ex):
        a, b, c = (o[:n2x, r:r + 1] for o in tall)
        c2[r] = jnp.where(lane < tz, a, jnp.where(lane < 2 * tz, b, c))
    i, j = grids(LANES, LANES)
    src = i - jnp.where(i < tz, 0, jnp.where(i < 2 * tz, tz, 2 * tz)) - 2
    put(pz2, None, cubic((j - 2) - 2 * src, (i < 3 * tz) & (src < fz + 3) & (j < top) & inside(gz * cz + j - 2, nz * cz)))
    i, j = grids(ry1, up(ty, 16))
    stack(py2, cubic((i - 2) - 2 * (j - 2), (j < ey) & (i < cy + 4) & inside(gy * cy + i - 2, ny * cy)), 2)
    i, j = grids(LANES, bz)
    put(pz1, None, cubic(j - 2 * (i - 2), i < top))
    i, j = grids(by, up(ry1, 16))
    stack(py1, cubic(i - 2 * (j - 2), j < cy + 4), 2)

    arrive(xa)
    start(za[2:])
    arrive(za)

    wide = by + 16
    has_r, has_l = there(0, 0, 1), there(0, 0, -1)
    mask_r, mask_l = (lane < LANES // 2) & has_r, (lane >= LANES // 2) & has_l
    step0 = 4

    @pl.loop(0, (bx + 16) // step0)
    def _(c):
        at = pl.ds(c * step0, step0)
        own = e0[at].reshape(step0 * wide, LANES)
        other = jnp.where(
            mask_r, r0[at].reshape(step0 * wide, LANES),
            jnp.where(mask_l, l0[at].reshape(step0 * wide, LANES), 0.0),
        )
        v = dot_right(jnp.concatenate([own, other], axis=1), (w0h, w0l))
        for k in range(step0):
            o = dot_left(m0, v[k * wide:(k + 1) * wide], 3)
            y0[c * step0 + k] = o[:by, :LANES]
            y1[c * step0 + k] = o[by:, LANES:]

    def restrict_x(ref, at):
        return (
            ref[at] + 0.5625 * (ref[at - 1] + ref[at + 1]) - 0.0625 * (ref[at - 3] + ref[at + 3])
        )

    @pl.loop(0, cx // 2)
    def _(p):
        a = restrict_x(y1, 8 + 4 * p)
        b = restrict_x(y1, 10 + 4 * p)
        t1[p] = jnp.where(lane < cz, a, pltpu.roll(b, cz, 1))

    own_copy = pltpu.make_async_copy(t1, e1.at[pl.ds(5, cx // 2), pl.ds(16, cy), :], sg.at[3, 0])
    own_copy.start()
    own_copy.wait()
    xb = exchange(e1, (5, 16), e1, 5, 16, cx // 2, cy, sb, rb)
    zb = across(e1, e1, l1, r1, pieces(5, 16, cx // 2, cy, False), szb, rzb)
    start(xb)
    start(zb[:2])

    @pl.loop(0, bx)
    def _(p):
        acc = taps[0, 0, 0] * y0[p]
        for t in range(1, 17):
            acc = acc + taps[0, 0, t] * y0[p + t]
        out_ref[p] = acc

    arrive(xb)
    start(zb[2:])
    arrive(zb)

    half = lax.rem(lane, cz) < cz // 2

    @pl.loop(0, cx // 2 + 10)
    def _(p):
        own = e1[p]
        other = jnp.where(half & has_r, r1[p], jnp.where(jnp.logical_not(half) & has_l, l1[p], 0.0))
        even = jnp.where(lane < cz, own, pltpu.roll(other, cz, 1))
        odd = jnp.where(lane < cz, pltpu.roll(own, cz, 1), other)
        h = own.shape[0]
        v = dot_right(jnp.concatenate([even, odd], axis=0), (w1h, w1l))
        o = dot_left(m1, jnp.concatenate([v[:h], v[h:]], axis=1), 3)
        s1[2 * p] = o[:, :LANES]
        s1[2 * p + 1] = o[:, LANES:]

    per = LANES // fz
    def restrict_1(q):
        at = 10 + 2 * q
        rows = pl.ds(ry1, fy)
        v = (
            s1[at, rows] + 0.5625 * (s1[at - 1, rows] + s1[at + 1, rows])
            - 0.0625 * (s1[at - 3, rows] + s1[at + 3, rows])
        )
        return jnp.where(lane >= rlane, v, 0.0)

    np2 = fx // per
    for p in range(np2):
        acc = None
        for k in range(per):
            v = restrict_1(p * per + k)
            sh = (fz * k + LANES - rlane) % LANES
            v = pltpu.roll(v, sh, 1) if sh else v
            acc = v if acc is None else acc + v
        p2[p] = acc
    own_copy = pltpu.make_async_copy(p2, g2.at[gz, gy, pl.ds(gx * np2, np2)], sg.at[3, 1])
    own_copy.start()
    own_copy.wait()

    def spread(dim, n, ref, k0):
        out = []
        for m, d in enumerate([d for d in range(-(n - 1), n) if d]):
            dev = tuple(here[k] + (d if k == dim else 0) for k in range(3))
            copy = pltpu.make_async_remote_copy(
                src_ref=ref(here[dim]), dst_ref=ref(here[dim]),
                send_sem=sg.at[dim, m], recv_sem=rg.at[dim, m],
                device_id=dev, device_id_type=pl.DeviceIdType.MESH,
            )
            land = pltpu.make_async_remote_copy(
                src_ref=ref(here[dim]), dst_ref=ref(here[dim] - d),
                send_sem=sg.at[dim, m], recv_sem=rg.at[dim, m],
                device_id=dev, device_id_type=pl.DeviceIdType.MESH,
            )
            to = inside(here[dim] + d, n)
            fro = inside(here[dim] - d, n)
            out.append((to, fro, copy, land))
        return out

    def begin(copies):
        for to, _, copy, _ in copies:
            pl.when(to)(copy.start)

    def landed(copies):
        for _, fro, _, land in copies:
            pl.when(fro)(land.wait_recv)

    ca = spread(0, nx, lambda k: g2.at[gz, gy, pl.ds(k * np2, np2)], 0)
    begin(ca)
    seen = lambda r: inside(gx * cx + r - 2, nx * cx).astype(F32)

    @pl.loop(0, cx + 4)
    def _(p):
        rows = pl.ds(0, ry1)
        acc = taps[1, 0, 0] * s1[p, rows]
        for t in range(1, 17):
            acc = acc + taps[1, 0, t] * s1[p + t, rows]
        d1[p] = acc
    landed(ca)
    cb = spread(1, ny, lambda k: g2.at[gz, k], 0)
    begin(cb)
    landed(cb)
    cc = spread(2, nz, lambda k: g2.at[k], 0)
    begin(cc)
    landed(cc)

    tiles = u2.shape[0]

    @pl.loop(0, nx * np2)
    def _(p):
        for b in range(ny):
            for k in range(per):
                for t in range(tiles):
                    acc = jnp.zeros((fy, LANES), F32)
                    for s in range(t * per, min(nz, (t + 1) * per)):
                        v = g2[s, b, p]
                        sh = (fz * (s - t * per - k)) % LANES
                        v = pltpu.roll(v, sh, 1) if sh else v
                        lo = fz * (s - t * per)
                        acc = jnp.where((lane >= lo) & (lane < lo + fz), v, acc)
                    u2[t, p * per + k, pl.ds(b * fy, fy), :] = acc

    step2 = 2

    @pl.loop(0, n2x // step2)
    def _(c):
        at = pl.ds(c * step2, step2)
        v = jnp.concatenate([u2[t, at].reshape(step2 * n2y, LANES) for t in range(tiles)], axis=1)
        v = dot_right(v, (w2h, w2l))
        v = jnp.concatenate([v[k * n2y:(k + 1) * n2y] for k in range(step2)], axis=1)
        o = dot_left(m2, v, 3)
        for k in range(step2):
            w = o[:, k * LANES:(k + 1) * LANES]
            y2[c * step2 + k] = jnp.where(
                lane < tz, w[:ty], jnp.where(lane < 2 * tz, w[ty:2 * ty], w[2 * ty:])
            )

    parts = []
    for r in range(ex):
        acc = c2[r, pl.ds(0, 1)] * y2[0]
        for q in range(1, n2x):
            acc = acc + c2[r, pl.ds(q, 1)] * y2[q]
        parts.append(acc)
    v = dot_right(jnp.concatenate(parts, axis=0), (pz2, None))
    fill = up(ty, 16) - ty
    pro = []
    for r in range(ex):
        w = v[r * ty:(r + 1) * ty]
        if fill:
            w = jnp.concatenate([w, jnp.zeros((fill, LANES), F32)], axis=0)
        pro.append(dot_left(py2, w, 2))
    for p in range(cx + 4):
        m = (p - 2) // 2 + 2
        if p % 2 == 0:
            w = pro[m]
        else:
            w = 0.5625 * (pro[m] + pro[m + 1]) - 0.0625 * (pro[m - 1] + pro[m + 2])
        d1[p] = (d1[p] + w) * seen(p)

    fill1 = up(ry1, 16) - ry1

    @pl.loop(0, (cx + 4) // 2)
    def _(c):
        v = dot_right(d1[pl.ds(2 * c, 2)].reshape(2 * ry1, LANES), (pz1, None))
        v = jnp.concatenate([v[:ry1], v[ry1:]], axis=1)
        if fill1:
            v = jnp.concatenate([v, jnp.zeros((fill1, 2 * LANES), F32)], axis=0)
        o = dot_left(py1, v, 2)
        y0[2 * c] = o[:, :LANES]
        y0[2 * c + 1] = o[:, LANES:]

    @pl.loop(0, cx)
    def _(m):
        at = m + 2
        out_ref[2 * m] = out_ref[2 * m] + y0[at]
        out_ref[2 * m + 1] = out_ref[2 * m + 1] + (
            0.5625 * (y0[at] + y0[at + 1]) - 0.0625 * (y0[at - 1] + y0[at + 2])
        )

    for group in (xa, za, xb, zb):
        left_over(group)
    for group in (ca, cb, cc):
        for to, _, copy, _ in group:
            pl.when(to)(copy.wait_send)


def per_device(counts, charges, kernel_taps):
    nx, ny, nz = counts
    bx, by, bz = dims = charges.shape
    assert bz == LANES
    cx, cy, cz = bx // 2, by // 2, bz // 2
    fx, fy, fz = bx // 4, by // 4, bz // 4
    n2x, n2y, n2z = nx * fx, ny * fy, nz * fz
    np2 = fx // (LANES // fz)
    ry1 = up(cy + 4, 8)
    ty = up(fy + 5, 8)
    tiles = up(n2z, LANES) // LANES
    V = pltpu.VMEM
    ext0 = (bx + 16, by + 16, LANES)
    ext1 = (cx // 2 + 10, cy + 32, LANES)
    wide = max(nx, ny, nz) * 2
    dma = pltpu.SemaphoreType.DMA
    scratch = [
        V(ext0, F32), V(ext0, F32), V(ext0, F32),
        V((bx + 16, by, LANES), F32), V((bx + 16, cy, LANES), F32),
        V(ext1, F32), V(ext1, F32), V(ext1, F32),
        V((cx // 2, cy, LANES), F32),
        V((cx + 20, ry1 + fy, LANES), F32),
        V((nz, ny, nx * np2, fy, LANES), F32),
        V((tiles, n2x, n2y, LANES), F32),
        V((n2x, ty, LANES), F32), V((np2, fy, LANES), F32), V((cx + 4, ry1, LANES), F32),
        V((2 * bz, bz + LANES), BF16), V((2 * bz, bz + LANES), BF16),
        V((by + cy, 3 * (by + 16)), BF16),
        V((2 * cz, LANES), BF16), V((2 * cz, LANES), BF16),
        V((ry1 + fy, 3 * (cy + 32)), BF16),
        V((tiles * LANES, LANES), BF16), V((tiles * LANES, LANES), BF16),
        V((3 * ty, 3 * n2y), BF16),
        V((fx + 5, n2x, LANES), F32),
        V((LANES, LANES), BF16), V((ry1, 2 * up(ty, 16)), BF16),
        V((LANES, bz), BF16), V((by, 2 * up(ry1, 16)), BF16),
        dma((8,)), dma((8,)), dma((5, 2)), dma((5, 2)),
        dma((8,)), dma((8,)), dma((5, 2)), dma((5, 2)),
        dma((4, wide)), dma((3, wide)),
    ]
    return pl.pallas_call(
        functools.partial(kernel, counts, dims),
        out_shape=jax.ShapeDtypeStruct(dims, F32),
        in_specs=[pl.BlockSpec(memory_space=pltpu.SMEM), pl.BlockSpec(memory_space=pltpu.VMEM)],
        out_specs=pl.BlockSpec(memory_space=pltpu.VMEM),
        scratch_shapes=scratch,
        compiler_params=pltpu.CompilerParams(
            collective_id=0, has_side_effects=True, vmem_limit_bytes=60 * 2**20
        ),
    )(kernel_taps, charges)


def solution(mesh):
    counts = tuple(mesh.shape[a] for a in AXES)
    return jax.shard_map(
        functools.partial(per_device, counts), mesh=mesh,
        in_specs=(P("gx", "gy", "gz"), P()), out_specs=P("gx", "gy", "gz"), check_vma=False,
    )
```

```python
import functools

import jax
import jax.numpy as jnp
from jax import lax
from jax.experimental import pallas as pl
from jax.experimental.pallas import tpu as pltpu
from jax.sharding import PartitionSpec as P

F32, BF16 = jnp.float32, jnp.bfloat16
LANES = 128
AXES = ("gx", "gy", "gz")
ODD = (-0.0625, 0.5625, 0.5625, -0.0625)
SIDES = tuple((a, b) for a in (-1, 0, 1) for b in (-1, 0, 1) if (a, b) != (0, 0))


def split(v):
    hi = v.astype(BF16)
    return hi, (v - hi.astype(F32)).astype(BF16)


def mm(a, b):
    return jnp.dot(a, b, preferred_element_type=F32)


def exact(a, b):
    return jnp.dot(a, b, preferred_element_type=F32, precision=lax.Precision.HIGHEST)


def dot_right(v, w):
    hi, lo = split(v)
    out = mm(hi, w[0][...]) + mm(lo, w[0][...])
    return out if w[1] is None else out + mm(hi, w[1][...])


def dot_left(w_ref, v, terms):
    hi, lo = split(v)
    return mm(w_ref[...], jnp.concatenate([hi, lo, hi][:terms], axis=0))


def grids(rows, cols):
    return (
        lax.broadcasted_iota(jnp.int32, (rows, cols), 0),
        lax.broadcasted_iota(jnp.int32, (rows, cols), 1),
    )


def pick(taps, level, axis, diff, ok):
    out = jnp.zeros(diff.shape, F32)
    for t in range(17):
        out = jnp.where(diff == t, taps[level, axis, t], out)
    return jnp.where(ok, out, 0.0)


def cubic(diff, ok):
    d = jnp.abs(diff)
    out = jnp.where(d == 0, 1.0, jnp.where(d == 1, 0.5625, jnp.where(d == 3, -0.0625, 0.0)))
    return jnp.where(ok, out, 0.0).astype(F32)


def up(n, m):
    return -(-n // m) * m


def inside(v, n):
    return (v >= 0) & (v < n)


def kernel(counts, dims, taps, x_ref, out_ref, e0, l0, r0, y0, y1, e1, l1, r1, t1, s1, g2, u2, y2, p2, d1,
           w0h, w0l, m0, w1h, w1l, m1, w2h, w2l, m2, c2, pz2, py2, pz1, py1,
           sa, ra, sza, rza, sb, rb, szb, rzb, sg, rg):
    nx, ny, nz = counts
    bx, by, bz = dims
    here = tuple(lax.axis_index(a) for a in AXES)
    gx, gy, gz = here
    cx, cy, cz = bx // 2, by // 2, bz // 2
    fx, fy, fz = bx // 4, by // 4, bz // 4

    def there(dx, dy, dz):
        return inside(gx + dx, nx) & inside(gy + dy, ny) & inside(gz + dz, nz)

    partners = [(a, b, 0) for a, b in SIDES] + [(0, 0, -1), (0, 0, 1)]
    for dim, n in enumerate(counts):
        for d in range(2, n):
            for sgn in (-d, d):
                partners.append(tuple(sgn if k == dim else 0 for k in range(3)))
    barrier = pltpu.get_barrier_semaphore()
    total = jnp.int32(0)
    for p in partners:
        ok = there(*p)
        total = total + ok.astype(jnp.int32)

        @pl.when(ok)
        def _(p=p):
            pl.semaphore_signal(
                barrier, inc=1, device_id=(gx + p[0], gy + p[1], gz + p[2]),
                device_id_type=pl.DeviceIdType.MESH,
            )

    def zero_halo(ref, wx, wy, mx, my):
        for a, b in SIDES:
            @pl.when(jnp.logical_not(there(a, b, 0)))
            def _(a=a, b=b):
                xs = {-1: (0, wx), 0: (wx, mx), 1: (wx + mx, wx)}[a]
                ys = {-1: (0, wy), 0: (wy, my), 1: (wy + my, wy)}[b]
                ref[pl.ds(*xs), pl.ds(*ys), :] = jnp.zeros((xs[1], ys[1], LANES), F32)

    zero_halo(e0, 8, 8, bx, by)
    zero_halo(e1, 5, 16, cx // 2, cy)
    pl.semaphore_wait(barrier, total)

    def exchange(src, base, ref, wx, wy, mx, my, send, recv, near, far=False):
        out = []
        for k, (a, b) in enumerate(SIDES):
            if far and a == 0:
                continue
            rest_x = wx - near
            if far:
                sx = {-1: (near, rest_x), 1: (mx - wx, rest_x)}[a]
                tx = {-1: (wx + mx + near, rest_x), 1: (0, rest_x)}[a]
            else:
                sx = {-1: (0, near), 0: (0, mx), 1: (mx - near, near)}[a]
                tx = {-1: (wx + mx, near), 0: (wx, mx), 1: (wx - near, near)}[a]
            k += len(SIDES) if far else 0
            sy = {-1: (0, wy), 0: (0, my), 1: (my - wy, wy)}[b]
            ty = {-1: (wy + my, wy), 0: (wy, my), 1: (0, wy)}[b]
            copy = pltpu.make_async_remote_copy(
                src_ref=src.at[pl.ds(base[0] + sx[0], sx[1]), pl.ds(base[1] + sy[0], sy[1]), :],
                dst_ref=ref.at[pl.ds(*tx), pl.ds(*ty), :],
                send_sem=send.at[k], recv_sem=recv.at[k],
                device_id=(gx + a, gy + b, gz), device_id_type=pl.DeviceIdType.MESH,
            )
            out.append((there(a, b, 0), there(-a, -b, 0), copy))
        return out

    def across(src, base, left, right, ranges, send, recv):
        out = []
        for k, (ofs, xs, ys) in enumerate(ranges):
            for h, (dz, dst) in enumerate(((1, left), (-1, right))):
                source = (src if k == 0 else base)
                copy = pltpu.make_async_remote_copy(
                    src_ref=source.at[pl.ds(xs[0] - ofs[0], xs[1]), pl.ds(ys[0] - ofs[1], ys[1]), :],
                    dst_ref=dst.at[pl.ds(*xs), pl.ds(*ys), :],
                    send_sem=send.at[k, h], recv_sem=recv.at[k, h],
                    device_id=(gx, gy, gz + dz), device_id_type=pl.DeviceIdType.MESH,
                )
                out.append((there(0, 0, dz), there(0, 0, -dz), copy))
        return out

    def start(copies):
        for to, _, copy in copies:
            pl.when(to)(copy.start)

    def arrive(copies):
        for _, fro, copy in copies:
            pl.when(fro)(copy.wait_recv)

    def left_over(copies):
        for to, _, copy in copies:
            pl.when(to)(copy.wait_send)

    def pieces(wx, wy, mx, my, direct, near):
        o = (wx, wy) if direct else (0, 0)
        n = (0, 0)
        return [
            (o, (wx, mx), (wy, my)),
            (n, (wx - near, near), (0, my + 2 * wy)),
            (n, (wx + mx, near), (0, my + 2 * wy)),
            (n, (wx, mx), (0, wy)),
            (n, (wx, mx), (wy + my, wy)),
            (n, (0, wx - near), (0, my + 2 * wy)),
            (n, (wx + mx + near, wx - near), (0, my + 2 * wy)),
        ]

    xa = exchange(x_ref, (0, 0), e0, 8, 8, bx, by, sa, ra, 4)
    xa_far = exchange(x_ref, (0, 0), e0, 8, 8, bx, by, sa, ra, 4, True)
    za = across(x_ref, e0, l0, r0, pieces(8, 8, bx, by, True, 4), sza, rza)
    start(xa)
    start(za[:2])
    e0[pl.ds(8, bx), pl.ds(8, by), :] = x_ref[...]

    def put(h, l, v):
        hi, lo = split(v)
        h[...] = hi
        if l is not None:
            l[...] = lo

    def stack(ref, v, terms):
        hi, lo = split(v)
        ref[...] = jnp.concatenate([hi, hi, lo][:terms], axis=1)

    i, j = grids(2 * bz, bz)
    pos = jnp.where(i < bz + bz // 2, i, i - 2 * bz)
    k0 = pick(taps, 0, 2, pos - j + 8, inside(pos, bz + 8) | inside(pos + 8, 8))
    rz = cubic(pos - 2 * j, j < cz)
    put(w0h, w0l, jnp.concatenate([k0, rz], axis=1))
    i, j = grids(by + cy, by + 16)
    stack(m0, jnp.where(i < by, pick(taps, 0, 1, j - i, i < by), cubic(j - 8 - 2 * (i - by), i >= by)), 3)
    lane = lax.broadcasted_iota(jnp.int32, (1, LANES), 1)
    flat = [k for k, (a, _) in enumerate(SIDES) if a == 0]
    tilted = [k for k, (a, _) in enumerate(SIDES) if a != 0]
    arrive([xa[k] for k in flat])
    start(za[6:10])
    arrive(za[:2] + za[6:10])

    wide = by + 16
    has_r, has_l = there(0, 0, 1), there(0, 0, -1)
    mask_r, mask_l = (lane < LANES // 2) & has_r, (lane >= LANES // 2) & has_l
    step0 = 4

    def level0(c):
        at = pl.ds(c * step0, step0)
        own = e0[at].reshape(step0 * wide, LANES)
        other = jnp.where(
            mask_r, r0[at].reshape(step0 * wide, LANES),
            jnp.where(mask_l, l0[at].reshape(step0 * wide, LANES), 0.0),
        )
        v = dot_right(jnp.concatenate([own, other], axis=1), (w0h, w0l))
        for k in range(step0):
            o = dot_left(m0, v[k * wide:(k + 1) * wide], 3)
            y0[c * step0 + k] = o[:by, :LANES]
            y1[c * step0 + k] = o[by:, LANES:]

    pl.loop(8 // step0, (8 + bx) // step0)(level0)
    arrive([xa[k] for k in tilted])
    start(za[2:6])
    arrive(za[2:6])
    level0(4 // step0)
    level0((8 + bx) // step0)

    def restrict_x(ref, at):
        return (
            ref[at] + 0.5625 * (ref[at - 1] + ref[at + 1]) - 0.0625 * (ref[at - 3] + ref[at + 3])
        )

    @pl.loop(0, cx // 2)
    def _(p):
        a = restrict_x(y1, 8 + 4 * p)
        b = restrict_x(y1, 10 + 4 * p)
        t1[p] = jnp.where(lane < cz, a, pltpu.roll(b, cz, 1))

    own_copy = pltpu.make_async_copy(t1, e1.at[pl.ds(5, cx // 2), pl.ds(16, cy), :], sg.at[3, 0])
    own_copy.start()
    own_copy.wait()
    xb = exchange(e1, (5, 16), e1, 5, 16, cx // 2, cy, sb, rb, 2)
    xb_far = exchange(e1, (5, 16), e1, 5, 16, cx // 2, cy, sb, rb, 2, True)
    zb = across(e1, e1, l1, r1, pieces(5, 16, cx // 2, cy, False, 2), szb, rzb)
    start(xb)
    start(zb[:2])

    i, j = grids(2 * cz, LANES)
    pos = jnp.where(i < cz + cz // 2, i, i - 2 * cz)
    kk = j - 2
    top = cz + 4
    ok = (j < top) & inside(gz * cz + kk, nz * cz)
    rlane = LANES - fz
    put(w1h, w1l, pick(taps, 1, 2, pos - kk + 8, ok) + cubic(pos - 2 * (j - rlane), j >= rlane))
    ry1 = up(cy + 4, 8)
    i, j = grids(ry1 + fy, cy + 32)
    ok = (i < cy + 4) & inside(gy * cy + i - 2, ny * cy)
    stack(m1, pick(taps, 1, 1, j - 16 - (i - 2) + 8, ok) + cubic(j - 16 - 2 * (i - ry1), i >= ry1), 3)

    arrive([xb[k] for k in flat])
    start(zb[6:10])
    arrive(zb[:2] + zb[6:10])

    half = lax.rem(lane, cz) < cz // 2

    def level1(p):
        own = e1[p]
        other = jnp.where(half & has_r, r1[p], jnp.where(jnp.logical_not(half) & has_l, l1[p], 0.0))
        even = jnp.where(lane < cz, own, pltpu.roll(other, cz, 1))
        odd = jnp.where(lane < cz, pltpu.roll(own, cz, 1), other)
        h = own.shape[0]
        v = dot_right(jnp.concatenate([even, odd], axis=0), (w1h, w1l))
        o = dot_left(m1, jnp.concatenate([v[:h], v[h:]], axis=1), 3)
        s1[2 * p] = o[:, :LANES]
        s1[2 * p + 1] = o[:, LANES:]

    pl.loop(5, 5 + cx // 2)(level1)
    arrive([xb[k] for k in tilted])
    start(zb[2:6])
    arrive(zb[2:6])
    pl.loop(3, 5)(level1)
    pl.loop(5 + cx // 2, 7 + cx // 2)(level1)

    per = LANES // fz
    def restrict_1(q):
        at = 10 + 2 * q
        rows = pl.ds(ry1, fy)
        v = (
            s1[at, rows] + 0.5625 * (s1[at - 1, rows] + s1[at + 1, rows])
            - 0.0625 * (s1[at - 3, rows] + s1[at + 3, rows])
        )
        return jnp.where(lane >= rlane, v, 0.0)

    np2 = fx // per
    for p in range(np2):
        acc = None
        for k in range(per):
            v = restrict_1(p * per + k)
            sh = (fz * k + LANES - rlane) % LANES
            v = pltpu.roll(v, sh, 1) if sh else v
            acc = v if acc is None else acc + v
        p2[p] = acc
    own_copy = pltpu.make_async_copy(p2, g2.at[gz, gy, pl.ds(gx * np2, np2)], sg.at[3, 1])
    own_copy.start()
    own_copy.wait()

    def spread(dim, n, ref, k0):
        out = []
        for m, d in enumerate([d for d in range(-(n - 1), n) if d]):
            dev = tuple(here[k] + (d if k == dim else 0) for k in range(3))
            copy = pltpu.make_async_remote_copy(
                src_ref=ref(here[dim]), dst_ref=ref(here[dim]),
                send_sem=sg.at[dim, m], recv_sem=rg.at[dim, m],
                device_id=dev, device_id_type=pl.DeviceIdType.MESH,
            )
            land = pltpu.make_async_remote_copy(
                src_ref=ref(here[dim]), dst_ref=ref(here[dim] - d),
                send_sem=sg.at[dim, m], recv_sem=rg.at[dim, m],
                device_id=dev, device_id_type=pl.DeviceIdType.MESH,
            )
            to = inside(here[dim] + d, n)
            fro = inside(here[dim] - d, n)
            out.append((to, fro, copy, land))
        return out

    def begin(copies):
        for to, _, copy, _ in copies:
            pl.when(to)(copy.start)

    def landed(copies):
        for _, fro, _, land in copies:
            pl.when(fro)(land.wait_recv)

    ca = spread(0, nx, lambda k: g2.at[gz, gy, pl.ds(k * np2, np2)], 0)
    begin(ca)
    start(xa_far)
    start(xb_far)
    def plain(axis, level, n, pad, turned):
        i, j = grids(pad, pad)
        d = (i - j if turned else j - i) + 8
        return pick(taps, level, axis, d, (i < n) & (j < n))

    def rest(n, pad, big, turned_r):
        i, j = grids(*((big, pad) if turned_r else (pad, big)))
        c, f = (j, i) if turned_r else (i, j)
        return cubic(f - 2 * c, (c < n) & (f < 2 * n))

    def operators(axis, n2, first, rows, count):
        n3, n4 = n2 // 2, n2 // 4
        q = up(n2, LANES)
        i, j = grids(rows, q)
        g = first + i
        ok = (i < count) & inside(g, n2)
        one = pick(taps, 2, axis, j - g + 8, ok & (j < n2))
        pr = cubic(g - 2 * j, ok & (j < n3))
        r23, r34 = rest(n3, q, q, False), rest(n4, q, q, False)
        p34 = rest(n4, q, q, True)
        two = exact(exact(pr, plain(axis, 3, n3, q, False)), r23)
        three = exact(exact(exact(exact(pr, p34), plain(axis, 4, n4, q, False)), r34), r23)
        return one, two, three

    n2x, n2y, n2z = nx * fx, ny * fy, nz * fz
    ez, ey, ex = fz + 5, fy + 5, fx + 5
    tz = 40
    ops = operators(2, n2z, gz * fz - 2, tz, ez)
    cols = jnp.concatenate(list(ops) + [jnp.zeros((LANES - 3 * tz, ops[0].shape[1]), F32)], axis=0)
    put(w2h, w2l, cols.T)
    ty = up(ey, 8)
    ops = operators(1, n2y, gy * fy - 2, ty, ey)
    stack(m2, jnp.concatenate(list(ops), axis=0)[:, :n2y], 3)
    tx = up(ex, 8)
    ops = operators(0, n2x, gx * fx - 2, tx, ex)
    tall = [o.T for o in ops]
    for r in range(ex):
        a, b, c = (o[:n2x, r:r + 1] for o in tall)
        c2[r] = jnp.where(lane < tz, a, jnp.where(lane < 2 * tz, b, c))
    i, j = grids(LANES, LANES)
    src = i - jnp.where(i < tz, 0, jnp.where(i < 2 * tz, tz, 2 * tz)) - 2
    put(pz2, None, cubic((j - 2) - 2 * src, (i < 3 * tz) & (src < fz + 3) & (j < top) & inside(gz * cz + j - 2, nz * cz)))
    i, j = grids(ry1, up(ty, 16))
    stack(py2, cubic((i - 2) - 2 * (j - 2), (j < ey) & (i < cy + 4) & inside(gy * cy + i - 2, ny * cy)), 2)
    i, j = grids(LANES, bz)
    put(pz1, None, cubic(j - 2 * (i - 2), i < top))
    i, j = grids(by, up(ry1, 16))
    stack(py1, cubic(i - 2 * (j - 2), j < cy + 4), 2)

    landed(ca)
    cb = spread(1, ny, lambda k: g2.at[gz, k], 0)
    begin(cb)
    arrive(xa_far)
    start(za[10:])
    arrive(xb_far)
    start(zb[10:])
    arrive(za[10:])
    level0(0)
    level0((12 + bx) // step0)
    arrive(zb[10:])
    pl.loop(0, 3)(level1)
    pl.loop(7 + cx // 2, 10 + cx // 2)(level1)

    seen = lambda r: inside(gx * cx + r - 2, nx * cx).astype(F32)

    @pl.loop(0, cx + 4)
    def _(p):
        rows = pl.ds(0, ry1)
        acc = taps[1, 0, 0] * s1[p, rows]
        for t in range(1, 17):
            acc = acc + taps[1, 0, t] * s1[p + t, rows]
        d1[p] = acc

    @pl.loop(0, bx)
    def _(p):
        acc = taps[0, 0, 0] * y0[p]
        for t in range(1, 17):
            acc = acc + taps[0, 0, t] * y0[p + t]
        out_ref[p] = acc

    landed(cb)
    cc = spread(2, nz, lambda k: g2.at[k], 0)
    begin(cc)
    landed(cc)

    tiles = u2.shape[0]

    @pl.loop(0, nx * np2)
    def _(p):
        for b in range(ny):
            for k in range(per):
                for t in range(tiles):
                    acc = jnp.zeros((fy, LANES), F32)
                    for s in range(t * per, min(nz, (t + 1) * per)):
                        v = g2[s, b, p]
                        sh = (fz * (s - t * per - k)) % LANES
                        v = pltpu.roll(v, sh, 1) if sh else v
                        lo = fz * (s - t * per)
                        acc = jnp.where((lane >= lo) & (lane < lo + fz), v, acc)
                    u2[t, p * per + k, pl.ds(b * fy, fy), :] = acc

    step2 = 2

    @pl.loop(0, n2x // step2)
    def _(c):
        at = pl.ds(c * step2, step2)
        v = jnp.concatenate([u2[t, at].reshape(step2 * n2y, LANES) for t in range(tiles)], axis=1)
        v = dot_right(v, (w2h, w2l))
        v = jnp.concatenate([v[k * n2y:(k + 1) * n2y] for k in range(step2)], axis=1)
        o = dot_left(m2, v, 3)
        for k in range(step2):
            w = o[:, k * LANES:(k + 1) * LANES]
            y2[c * step2 + k] = jnp.where(
                lane < tz, w[:ty], jnp.where(lane < 2 * tz, w[ty:2 * ty], w[2 * ty:])
            )

    parts = []
    for r in range(ex):
        acc = c2[r, pl.ds(0, 1)] * y2[0]
        for q in range(1, n2x):
            acc = acc + c2[r, pl.ds(q, 1)] * y2[q]
        parts.append(acc)
    v = dot_right(jnp.concatenate(parts, axis=0), (pz2, None))
    fill = up(ty, 16) - ty
    pro = []
    for r in range(ex):
        w = v[r * ty:(r + 1) * ty]
        if fill:
            w = jnp.concatenate([w, jnp.zeros((fill, LANES), F32)], axis=0)
        pro.append(dot_left(py2, w, 2))
    for p in range(cx + 4):
        m = (p - 2) // 2 + 2
        if p % 2 == 0:
            w = pro[m]
        else:
            w = 0.5625 * (pro[m] + pro[m + 1]) - 0.0625 * (pro[m - 1] + pro[m + 2])
        d1[p] = (d1[p] + w) * seen(p)

    fill1 = up(ry1, 16) - ry1

    @pl.loop(0, (cx + 4) // 2)
    def _(c):
        v = dot_right(d1[pl.ds(2 * c, 2)].reshape(2 * ry1, LANES), (pz1, None))
        v = jnp.concatenate([v[:ry1], v[ry1:]], axis=1)
        if fill1:
            v = jnp.concatenate([v, jnp.zeros((fill1, 2 * LANES), F32)], axis=0)
        o = dot_left(py1, v, 2)
        y0[2 * c] = o[:, :LANES]
        y0[2 * c + 1] = o[:, LANES:]

    @pl.loop(0, cx)
    def _(m):
        at = m + 2
        out_ref[2 * m] = out_ref[2 * m] + y0[at]
        out_ref[2 * m + 1] = out_ref[2 * m + 1] + (
            0.5625 * (y0[at] + y0[at + 1]) - 0.0625 * (y0[at - 1] + y0[at + 2])
        )

    for group in (xa, xa_far, za, xb, xb_far, zb):
        left_over(group)
    for group in (ca, cb, cc):
        for to, _, copy, _ in group:
            pl.when(to)(copy.wait_send)


def per_device(counts, charges, kernel_taps):
    nx, ny, nz = counts
    bx, by, bz = dims = charges.shape
    assert bz == LANES
    cx, cy, cz = bx // 2, by // 2, bz // 2
    fx, fy, fz = bx // 4, by // 4, bz // 4
    n2x, n2y, n2z = nx * fx, ny * fy, nz * fz
    np2 = fx // (LANES // fz)
    ry1 = up(cy + 4, 8)
    ty = up(fy + 5, 8)
    tiles = up(n2z, LANES) // LANES
    V = pltpu.VMEM
    ext0 = (bx + 16, by + 16, LANES)
    ext1 = (cx // 2 + 10, cy + 32, LANES)
    wide = max(nx, ny, nz) * 2
    dma = pltpu.SemaphoreType.DMA
    scratch = [
        V(ext0, F32), V(ext0, F32), V(ext0, F32),
        V((bx + 16, by, LANES), F32), V((bx + 16, cy, LANES), F32),
        V(ext1, F32), V(ext1, F32), V(ext1, F32),
        V((cx // 2, cy, LANES), F32),
        V((cx + 20, ry1 + fy, LANES), F32),
        V((nz, ny, nx * np2, fy, LANES), F32),
        V((tiles, n2x, n2y, LANES), F32),
        V((n2x, ty, LANES), F32), V((np2, fy, LANES), F32), V((cx + 4, ry1, LANES), F32),
        V((2 * bz, bz + LANES), BF16), V((2 * bz, bz + LANES), BF16),
        V((by + cy, 3 * (by + 16)), BF16),
        V((2 * cz, LANES), BF16), V((2 * cz, LANES), BF16),
        V((ry1 + fy, 3 * (cy + 32)), BF16),
        V((tiles * LANES, LANES), BF16), V((tiles * LANES, LANES), BF16),
        V((3 * ty, 3 * n2y), BF16),
        V((fx + 5, n2x, LANES), F32),
        V((LANES, LANES), BF16), V((ry1, 2 * up(ty, 16)), BF16),
        V((LANES, bz), BF16), V((by, 2 * up(ry1, 16)), BF16),
        dma((16,)), dma((16,)), dma((7, 2)), dma((7, 2)),
        dma((16,)), dma((16,)), dma((7, 2)), dma((7, 2)),
        dma((4, wide)), dma((3, wide)),
    ]
    return pl.pallas_call(
        functools.partial(kernel, counts, dims),
        out_shape=jax.ShapeDtypeStruct(dims, F32),
        in_specs=[pl.BlockSpec(memory_space=pltpu.SMEM), pl.BlockSpec(memory_space=pltpu.VMEM)],
        out_specs=pl.BlockSpec(memory_space=pltpu.VMEM),
        scratch_shapes=scratch,
        compiler_params=pltpu.CompilerParams(
            collective_id=0, has_side_effects=True, vmem_limit_bytes=60 * 2**20
        ),
    )(kernel_taps, charges)


def solution(mesh):
    counts = tuple(mesh.shape[a] for a in AXES)
    return jax.shard_map(
        functools.partial(per_device, counts), mesh=mesh,
        in_specs=(P("gx", "gy", "gz"), P()), out_specs=P("gx", "gy", "gz"), check_vma=False,
    )
```
